32 devices in a mesh: lib: 8 (over z, x), ctx: 2 (over core), head: 2 (over y).
Axes of the slice: x: 2, y: 2, z: 4, core: 2. Of those that a mesh axis runs over, the one named last changes fastest.
Arguments:
- queries: bfloat16 [8, 128, 2048], P('lib', None, 'head'), may hold values from -50 to 50
- passage_keys: bfloat16 [128, 512, 256], P('lib', 'ctx', 'head'), may hold values from -6 to 6
- passage_values: bfloat16 [128, 512, 256], P('lib', 'ctx', 'head'), may hold values from -6 to 6
- offsets: int32 [128], P('lib'), may hold values from 0 to 4095
- out_weight: bfloat16 [2048, 8192], P('head', 'lib'), may hold values from -0.5 to 0.5
- passage_list: int32 [8, 16], P('lib'), may hold values from 0 to 127, as said below
- targets: int32 [8, 16], P('lib'), may hold values from 0 to 8191
- row_counts: int32 [8], P('lib'), may hold values from 1 to 128
Outputs:
- output: bfloat16 [2, 512, 8192], P('ctx', 'head', 'lib')
The draws below stay inside these ranges and needn't reach their ends.
Inputs may be any that keep to these rules, and one draw needn't show every extreme that they name: `passage_list`: each row names 16 different passages; passage i belongs to owner i // 16; no row names more than 8 passages of one owner, and in every row some owner has exactly 8.
All inputs are finite; a program needn't handle non-finite values.
Results may differ from the reference program's by a relative error of at most 0.012.
The reference program's roundings to bfloat16 on the way count: a program that leaves them out, or rounds other values in their place, can miss the bound.
Values may be sent and summed in bfloat16 or wider, within the bound.
A program may use at most 64 MiB of HBM per device.

```python
import jax
import jax.numpy as jnp
from jax import lax

D = 8192
HEAD_DIM = 128
BLOCK = 512
LIST = 16
PASS_DEV = 16
ROWS = 128
KV_HEADS = 2
HEADS = 16
PROMPTS = 8
PASSAGES = 128
MOST = 8
N_CTX = 2


def draw_passage_list(key, part):
    slot_count = PROMPTS * MOST
    base = jax.random.fold_in(key, 17)
    first, second, third, fourth = jax.random.split(base, 4)
    popular = jax.random.randint(first, (PROMPTS,), 0, 4) * 262144
    noise = jax.random.randint(second, (PROMPTS, slot_count), 0, 262144)
    favored = jax.random.randint(third, (PROMPTS,), 0, PROMPTS)
    slot_owner = jnp.arange(slot_count, dtype=jnp.int32) // MOST
    boost = jnp.where(slot_owner[None, :] == favored[:, None], 1048576, 0)
    score = (noise + popular[slot_owner][None, :] + boost) * slot_count + jnp.arange(slot_count, dtype=jnp.int32)[None, :]
    unused, picked = lax.top_k(score, LIST)
    picked_owner = picked // MOST
    picked_copy = picked % MOST
    shuffle = jax.random.randint(fourth, (PROMPTS, PROMPTS, PASS_DEV), 0, 1048576) * PASS_DEV
    shuffle = shuffle + jnp.arange(PASS_DEV, dtype=jnp.int32)
    ranking = jnp.argsort(shuffle, axis=-1).astype(jnp.int32)
    within = ranking[jnp.arange(PROMPTS)[:, None], picked_owner, picked_copy]
    return (picked_owner * PASS_DEV + within).astype(jnp.int32)


def draw_queries(key, part):
    shape = (PROMPTS, ROWS, HEADS * HEAD_DIM)
    first = jax.random.fold_in(jax.random.fold_in(key, 23), 0)
    return jnp.clip(2.0 * jax.random.normal(first, shape, jnp.float32), -8.0, 8.0).astype(jnp.bfloat16)


def set_ends(array, own_key, low, high):
    longest = array.shape.index(max(array.shape))
    spots = []
    for shift in (0, 1):
        where = [jax.random.randint(jax.random.fold_in(own_key, axis), (), 0, length) for axis, length in enumerate(array.shape)]
        where[longest] = (where[longest] + shift) % array.shape[longest]
        spots.append(tuple(where))
    return array.at[spots[0]].set(low).at[spots[1]].set(high)


def shard_levels(key, extent, shards, smallest, top_value):
    def one(dim, blocks):
        heights = jax.random.uniform(jax.random.fold_in(jax.random.fold_in(key, 6), dim), (blocks,), jnp.float32, smallest / len(shards), top_value / len(shards))
        return jnp.repeat(jnp.exp(heights), extent[dim] // blocks).reshape((-1,) + (1,) * (len(extent) - dim - 1))

    loudness = one(*shards[0])
    for cut in shards[1:]:
        loudness = loudness * one(*cut)
    return loudness


def scatter_about(rng, shape, scale, limit, cuts=(), kind=jnp.bfloat16):
    values = jax.random.normal(rng, shape, jnp.float32) * scale
    if len(cuts) > 0:
        values = shard_levels(rng, shape, cuts, -0.22, 0.18) * values
    return jnp.clip(values, min=-limit, max=limit).astype(kind)


def setup_inputs(seed: int = 0) -> dict:
    arg_keys = jax.random.split(jax.random.key(seed), 9)
    queries = draw_queries(jax.random.fold_in(arg_keys[8], 71), 0)
    passage_keys = scatter_about(arg_keys[1], (PASSAGES, BLOCK, KV_HEADS * HEAD_DIM), 1.0, 6.0, ((0, 8), (1, 2), (2, 2)))
    passage_values = scatter_about(arg_keys[2], (PASSAGES, BLOCK, KV_HEADS * HEAD_DIM), 1.0, 6.0, ((0, 8), (1, 2), (2, 2)))
    offsets = set_ends(jax.random.randint(arg_keys[3], (PASSAGES,), 0, 8 * BLOCK), jax.random.fold_in(arg_keys[3], 1), 0, (8 * BLOCK) - 1).astype(jnp.int32)
    out_weight = scatter_about(arg_keys[4], (HEADS * HEAD_DIM, D), HEAD_DIM ** -0.5, 0.5, ((0, 2), (1, 8)))
    passage_list = draw_passage_list(jax.random.fold_in(arg_keys[8], 71), 0)
    targets = set_ends(jax.random.randint(arg_keys[6], (PROMPTS, LIST), 0, LIST * BLOCK), jax.random.fold_in(arg_keys[6], 1), 0, (LIST * BLOCK) - 1).astype(jnp.int32)
    row_counts = set_ends(jax.random.randint(arg_keys[7], (PROMPTS,), 1, ROWS + 1), jax.random.fold_in(arg_keys[7], 1), 1, ROWS).astype(jnp.int32)
    return {"queries": queries, "passage_keys": passage_keys, "passage_values": passage_values, "offsets": offsets, "out_weight": out_weight, "passage_list": passage_list, "targets": targets, "row_counts": row_counts}


theta_base = 500000.0


def rotate_keys(block, delta):
    width = block.shape[-1]
    half = width // 2
    inverse = theta_base ** (-2.0 * jnp.arange(half, dtype=jnp.float32) / width)
    angle = delta.astype(jnp.float32)[:, None] * inverse[None, :]
    cosine = jnp.cos(angle)[:, None, :]
    sine = jnp.sin(angle)[:, None, :]
    first = block[..., :half].astype(jnp.float32)
    second = block[..., half:].astype(jnp.float32)
    return jnp.concatenate([first * cosine - second * sine, second * cosine + first * sine], axis=-1)


def partial_softmax(query, keys, values):
    scores = lax.dot_general(query, keys, (((1,), (1,)), ((), ())), preferred_element_type=jnp.float32)
    scores = scores * (query.shape[1] ** -0.5)
    highest = jnp.max(scores, axis=1)
    weights = jnp.exp(scores - highest[:, None])
    totals = jnp.sum(weights, axis=1)
    summed = jnp.dot(weights.astype(jnp.bfloat16), values, preferred_element_type=jnp.float32)
    return highest, totals, summed


def combine(first, second):
    highest = jnp.maximum(first[0], second[0])
    early = jnp.exp(first[0] - highest)
    later = jnp.exp(second[0] - highest)
    return (highest, first[1] * early + second[1] * later,
            first[2] * early[..., None] + second[2] * later[..., None])


def reference(queries, passage_keys, passage_values, offsets, out_weight, passage_list, targets, row_counts):
    group = HEADS // KV_HEADS
    half = BLOCK // N_CTX

    def one_prompt(items):
        query, chosen, target, count = items
        delta = (target - offsets[chosen]).astype(jnp.int32)
        keys = passage_keys[chosen]
        values = passage_values[chosen]

        def one_head(head):
            key_head = lax.dynamic_slice_in_dim(keys, head * HEAD_DIM, HEAD_DIM, 2)
            value_head = lax.dynamic_slice_in_dim(values, head * HEAD_DIM, HEAD_DIM, 2)
            rotated = rotate_keys(key_head, delta).astype(jnp.bfloat16)
            query_rows = lax.dynamic_slice_in_dim(query, head * group * HEAD_DIM, group * HEAD_DIM, 1)
            query_rows = query_rows.reshape(ROWS * group, HEAD_DIM)
            state = None
            for index in range(N_CTX):
                piece_keys = rotated[:, index * half:(index + 1) * half].reshape(LIST * half, HEAD_DIM)
                piece_values = value_head[:, index * half:(index + 1) * half].reshape(LIST * half, HEAD_DIM)
                result = partial_softmax(query_rows, piece_keys, piece_values)
                state = result if state is None else combine(state, result)
            return (state[2] / state[1][:, None]).reshape(ROWS, group * HEAD_DIM)

        heads_out = lax.map(one_head, jnp.arange(KV_HEADS, dtype=jnp.int32))
        attended = jnp.transpose(heads_out, (1, 0, 2)).reshape(ROWS, HEADS * HEAD_DIM)
        live = (jnp.arange(ROWS, dtype=jnp.int32) < count)[:, None]
        return jnp.where(live, attended, jnp.zeros_like(attended)).astype(jnp.bfloat16)

    attended = lax.map(one_prompt, (queries, passage_list, targets, row_counts))

    def project(rows_in):
        return jnp.dot(rows_in, out_weight, preferred_element_type=jnp.float32).astype(jnp.bfloat16)

    projected = lax.map(project, attended)
    halves = projected.reshape(PROMPTS, N_CTX, ROWS // N_CTX, D)
    return jnp.transpose(halves, (1, 0, 2, 3)).reshape(N_CTX, PROMPTS * (ROWS // N_CTX), D)
```

```python
import functools

import jax
import jax.numpy as jnp
from jax import lax
from jax.experimental import pallas as pl
from jax.experimental.pallas import tpu as pltpu
from jax.sharding import PartitionSpec as P

MESH = pl.DeviceIdType.MESH
VMEM = pl.BlockSpec(memory_space=pltpu.VMEM)
SMEM = pl.BlockSpec(memory_space=pltpu.SMEM)
theta_base = 500000.0
log2_e = 1.4426950408889634
lowest = -1e30


def greet(peers):
    barrier = pltpu.get_barrier_semaphore()
    for peer in peers:
        pl.semaphore_signal(barrier, inc=1, device_id=peer, device_id_type=MESH)
    pl.semaphore_wait(barrier, len(peers))


def remote(source, target, sent, landed, peer):
    return pltpu.make_async_remote_copy(
        src_ref=source,
        dst_ref=target,
        send_sem=sent,
        recv_sem=landed,
        device_id=peer,
        device_id_type=MESH,
    )


class Grid:
    def __init__(self, owners):
        self.owners = owners
        self.inner = 2 if owners % 2 == 0 else 1
        self.outer = owners // self.inner
        self.me = lax.axis_index("lib")
        self.x = lax.rem(self.me, self.inner)
        self.z = lax.div(self.me, self.inner)

    def at(self, step_z, step_x):
        z = lax.rem(self.z + step_z + self.outer, self.outer)
        x = lax.rem(self.x + step_x + self.inner, self.inner)
        return z * self.inner + x


def gather_queries(owners, q_ref, meta_ref, all_q, all_meta, own_sem, sent, landed, shared, given,
                   meta_sent, meta_landed):
    grid = Grid(owners)
    me = grid.me
    core = lax.axis_index("ctx")
    other = 1 - core
    half = q_ref.shape[1] // 2
    mine = pl.ds(pl.multiple_of(core * half, half), half)
    theirs = pl.ds(pl.multiple_of(other * half, half), half)
    greet([{"lib": lax.rem(me + d, owners)} for d in range(1, owners)] + [{"ctx": other}])

    own = pltpu.make_async_copy(q_ref.at[0], all_q.at[me], own_sem.at[0])
    own.start()
    own_meta = pltpu.make_async_copy(meta_ref, all_meta.at[me], own_sem.at[1])
    own_meta.start()
    started = []
    for d in range(1, owners):
        copy = remote(meta_ref, all_meta.at[me], meta_sent.at[d], meta_landed.at[me],
                      {"lib": lax.rem(me + d, owners)})
        copy.start()
        started.append(copy)

    def send(source, prompt, slot, target):
        copy = remote(source, all_q.at[prompt, mine, :], sent.at[slot], landed.at[prompt],
                      {"lib": target})
        copy.start()
        started.append(copy)

    def wait_landed(prompt):
        remote(all_q.at[prompt, mine, :], all_q.at[prompt, mine, :], sent.at[0],
               landed.at[prompt], {"lib": me}).wait_recv()

    def share(prompt):
        copy = remote(all_q.at[prompt, mine, :], all_q.at[prompt, mine, :], given.at[prompt],
                      shared.at[prompt], {"ctx": other})
        copy.start()
        started.append(copy)

    slot = 0
    for dz in range(1, grid.outer):
        send(q_ref.at[0, mine, :], me, slot, grid.at(dz, 0))
        slot += 1
    for dx in range(1, grid.inner):
        send(q_ref.at[0, mine, :], me, slot, grid.at(0, dx))
        slot += 1
    for dz in range(1, grid.outer):
        prompt = grid.at(-dz, 0)
        wait_landed(prompt)
        for dx in range(1, grid.inner):
            send(all_q.at[prompt, mine, :], prompt, slot, grid.at(0, dx))
            slot += 1
        share(prompt)
    for dx in range(1, grid.inner):
        for dz in range(0, grid.outer):
            prompt = grid.at(-dz, -dx)
            wait_landed(prompt)
            share(prompt)
    own.wait()
    own_meta.wait()
    for d in range(1, owners):
        prompt = lax.rem(me + d, owners)
        remote(all_q.at[prompt, theirs, :], all_q.at[prompt, theirs, :], given.at[prompt],
               shared.at[prompt], {"ctx": other}).wait_recv()
        remote(meta_ref, all_meta.at[prompt], meta_sent.at[d], meta_landed.at[prompt],
               {"lib": me}).wait_recv()
    for copy in started:
        copy.wait_send()


def attend_blocks(listed_ref, q_ref, k_ref, v_ref, cos_ref, sin_ref, acc_ref, ml_ref, order):
    prompts, listed = listed_ref.shape
    rows = q_ref.shape[1]
    width = k_ref.shape[2]
    group = q_ref.shape[2] // width
    half = rows // 2
    heads_each = max(1, min(group, 256 // half))
    scale = width ** (-0.5) * log2_e

    def prompt_step(p, carry):
        def collect(k, count):
            order[count] = k
            return count + jnp.where(listed_ref[p, k] >= 0, 1, 0)

        count = lax.fori_loop(0, listed, collect, 0)
        acc_ref[p] = jnp.zeros(acc_ref.shape[1:], jnp.float32)
        place = lax.broadcasted_iota(jnp.int32, ml_ref.shape[1:], 1)
        ml_ref[p] = jnp.where(place == 0, lowest, 0.0)

        def block_step(j, carry):
            entry = order[j]
            i = listed_ref[p, entry]
            block = k_ref[i].astype(jnp.float32)
            turned = pltpu.roll(block, width // 2, 1)
            keys = (
                block * cos_ref[p, pl.ds(entry, 1), :] + turned * sin_ref[p, pl.ds(entry, 1), :]
            ).astype(jnp.bfloat16)
            values = v_ref[i]
            for part in range(2):
                for first in range(0, group, heads_each):
                    cols = slice(first * half, (first + heads_each) * half)
                    query = jnp.concatenate(
                        [
                            q_ref[p, part * half:(part + 1) * half, g * width:(g + 1) * width]
                            for g in range(first, first + heads_each)
                        ],
                        axis=0,
                    )
                    scores = lax.dot_general(
                        keys, query, (((1,), (1,)), ((), ())), preferred_element_type=jnp.float32
                    )
                    before = ml_ref[p, part, 0:1, cols]
                    highest = jnp.maximum(before, jnp.max(scores, axis=0, keepdims=True) * scale)
                    weights = jnp.exp2(scores * scale - highest)
                    fade = jnp.exp2(before - highest)
                    ml_ref[p, part, 0:1, cols] = highest
                    ml_ref[p, part, 1:2, cols] = ml_ref[p, part, 1:2, cols] * fade + jnp.sum(
                        weights, axis=0, keepdims=True
                    )
                    acc_ref[p, part, :, cols] = acc_ref[p, part, :, cols] * fade + lax.dot_general(
                        values,
                        weights.astype(jnp.bfloat16),
                        (((0,), (0,)), ((), ())),
                        preferred_element_type=jnp.float32,
                    )
            return carry

        lax.fori_loop(0, count, block_step, 0)
        return carry

    lax.fori_loop(0, prompts, prompt_step, 0)


def join(parts):
    highest = functools.reduce(jnp.maximum, [part[0] for part in parts])
    factors = [jnp.exp2(part[0] - highest) for part in parts]
    totals = sum(part[1] * factor for part, factor in zip(parts, factors))
    summed = sum(part[2].astype(jnp.float32) * factor for part, factor in zip(parts, factors))
    return highest, totals, summed


def finish(owners, heads, acc_ref, ml_ref, w_ref, live_ref, out_ref,
           pacc, pml, sbuf, sml, bbuf, bml, cbuf, cml, att, fbuf, pbuf, rbuf,
           a_sent, a_landed, b_sent, b_landed, c_sent, c_landed,
           d_sent, d_landed, f_sent, f_landed):
    grid = Grid(owners)
    me = grid.me
    core = lax.axis_index("ctx")
    head = lax.axis_index("head")
    other = 1 - core
    each = owners // heads
    half = att.shape[1]
    width = acc_ref.shape[2]
    group = att.shape[2] // width
    peers = [{"ctx": other}]
    peers += [{"lib": grid.at(0, dx)} for dx in range(1, grid.inner)]
    peers += [{"lib": grid.at(dz, 0)} for dz in range(1, grid.outer)]
    peers += [{"head": lax.rem(head + d, heads)} for d in range(1, heads)]
    greet(peers)
    started = []

    def launch(*args):
        copy = remote(*args)
        copy.start()
        started.append(copy)

    order = [(dz, dx) for dx in range(1, grid.inner) for dz in range(grid.outer)]
    order += [(dz, 0) for dz in range(1, grid.outer)] + [(0, 0)]
    for dz, dx in order:
        p = grid.at(dz, dx)
        launch(acc_ref.at[p, other], pacc.at[p], a_sent.at[0, p], a_landed.at[0, p], {"ctx": other})
        launch(ml_ref.at[p, other], pml.at[p], a_sent.at[1, p], a_landed.at[1, p], {"ctx": other})

    def store(slot, state):
        highest, totals, summed = state
        sbuf[slot] = summed.astype(jnp.bfloat16)
        sml[slot, 0:1] = highest
        sml[slot, 1:2] = totals

    def wait_into(target, landed):
        remote(target, target, landed, landed, {"ctx": other}).wait_recv()

    slot = 0
    for dz, dx in order:
        p = grid.at(dz, dx)
        wait_into(pacc.at[p], a_landed.at[0, p])
        wait_into(pml.at[p], a_landed.at[1, p])
        parts = [
            (ml_ref[p, core, 0:1], ml_ref[p, core, 1:2], acc_ref[p, core]),
            (pml[p, 0:1], pml[p, 1:2], pacc[p]),
        ]
        if dx == 0:
            for ex in range(grid.inner - 1):
                wait_into(bbuf.at[ex, dz], b_landed.at[0, ex, dz])
                wait_into(bml.at[ex, dz], b_landed.at[1, ex, dz])
                parts.append((bml[ex, dz, 0:1], bml[ex, dz, 1:2], bbuf[ex, dz]))
        if dz == 0 and dx == 0:
            for ez in range(grid.outer - 1):
                wait_into(cbuf.at[ez], c_landed.at[0, ez])
                wait_into(cml.at[ez], c_landed.at[1, ez])
                parts.append((cml[ez, 0:1], cml[ez, 1:2], cbuf[ez]))
        state = join(parts)
        if dx != 0:
            store(slot, state)
            peer = {"lib": grid.at(0, dx)}
            launch(sbuf.at[slot], bbuf.at[dx - 1, dz], b_sent.at[0, dx - 1, dz],
                   b_landed.at[0, dx - 1, dz], peer)
            launch(sml.at[slot], bml.at[dx - 1, dz], b_sent.at[1, dx - 1, dz],
                   b_landed.at[1, dx - 1, dz], peer)
            slot += 1
        elif dz != 0:
            store(slot, state)
            peer = {"lib": p}
            launch(sbuf.at[slot], cbuf.at[dz - 1], c_sent.at[0, dz - 1], c_landed.at[0, dz - 1], peer)
            launch(sml.at[slot], cml.at[dz - 1], c_sent.at[1, dz - 1], c_landed.at[1, dz - 1], peer)
            slot += 1
        else:
            mixed = state[2] / state[1]
            for g in range(group):
                rows = mixed[:, g * half:(g + 1) * half].T
                rows = jnp.where(live_ref[...] > 0, rows, 0.0)
                att[me, :, g * width:(g + 1) * width] = rows.astype(jnp.bfloat16)

    def spread(p, slot, target):
        launch(att.at[p], att.at[p], d_sent.at[slot], d_landed.at[p], {"lib": target})

    def project(p):
        share = jnp.dot(att[p], w_ref[...], preferred_element_type=jnp.float32)
        fbuf[p] = share
        pbuf[p] = share.astype(jnp.bfloat16)
        target = lax.div(p, each)
        local = lax.rem(p, each)
        away = lax.rem(target - head + heads, heads)

        @pl.when(away != 0)
        def _():
            remote(pbuf.at[p], rbuf.at[away - 1, local], f_sent.at[p],
                   f_landed.at[away - 1, local], {"head": target}).start()

    slot = 0
    for dz in range(1, grid.outer):
        spread(me, slot, grid.at(dz, 0))
        slot += 1
    for dx in range(1, grid.inner):
        spread(me, slot, grid.at(0, dx))
        slot += 1
    project(me)
    for dz in range(1, grid.outer):
        p = grid.at(-dz, 0)
        wait_into(att.at[p], d_landed.at[p])
        for dx in range(1, grid.inner):
            spread(p, slot, grid.at(0, dx))
            slot += 1
        project(p)
    for dx in range(1, grid.inner):
        for dz in range(grid.outer):
            p = grid.at(-dz, -dx)
            wait_into(att.at[p], d_landed.at[p])
            project(p)
    for local in range(each):
        p = head * each + local
        total = fbuf[p]
        for away in range(heads - 1):
            wait_into(rbuf.at[away, local], f_landed.at[away, local])
            total = total + rbuf[away, local].astype(jnp.float32)
        out_ref[0, local * half:(local + 1) * half] = total.astype(out_ref.dtype)
    for copy in started:
        copy.wait_send()
    for p in range(owners):
        @pl.when(p // each != head)
        def _():
            remote(pbuf.at[p], rbuf.at[0, 0], f_sent.at[p], f_sent.at[p], {"ctx": other}).wait_send()


def body(
    queries, passage_keys, passage_values, offsets, out_weight, passage_list, targets, row_counts
):
    owners = lax.axis_size("lib")
    heads = lax.axis_size("head")
    me = lax.axis_index("lib")
    pass_dev, _, width = passage_keys.shape
    listed = passage_list.shape[1]
    rows, features = queries.shape[1:]
    group = features // width
    half = rows // 2
    columns = out_weight.shape[1]
    inner = 2 if owners % 2 == 0 else 1
    outer = owners // inner
    dma = pltpu.SemaphoreType.DMA
    lanes = 128
    meta = jnp.pad(jnp.concatenate([passage_list, targets], axis=1), ((0, 0), (0, lanes - 2 * listed)))
    all_q, all_meta = pl.pallas_call(
        functools.partial(gather_queries, owners),
        out_shape=[
            jax.ShapeDtypeStruct((owners, rows, features), queries.dtype),
            jax.ShapeDtypeStruct((owners, 1, lanes), jnp.int32),
        ],
        in_specs=[VMEM, VMEM],
        out_specs=[VMEM, VMEM],
        scratch_shapes=[
            dma((2,)),
            dma((owners,)),
            dma((owners,)),
            dma((owners,)),
            dma((owners,)),
            dma((owners,)),
            dma((owners,)),
        ],
        compiler_params=pltpu.CompilerParams(collective_id=0, has_side_effects=True),
        name="gather_queries",
    )(queries, meta)
    chosen = all_meta[:, 0, :listed]
    local = chosen - me * pass_dev
    held = (local >= 0) & (local < pass_dev)
    lookup = local[:, :, None] == jnp.arange(pass_dev, dtype=jnp.int32)
    shift = all_meta[:, 0, listed:2 * listed] - jnp.sum(jnp.where(lookup, offsets, 0), axis=2)
    inverse = theta_base ** (-2.0 * jnp.arange(width // 2, dtype=jnp.float32) / width)
    angle = shift.astype(jnp.float32)[:, :, None] * inverse
    cosine = jnp.cos(angle)
    sine = jnp.sin(angle)
    acc, ml = pl.pallas_call(
        attend_blocks,
        out_shape=[
            jax.ShapeDtypeStruct((owners, 2, width, group * half), jnp.float32),
            jax.ShapeDtypeStruct((owners, 2, 8, group * half), jnp.float32),
        ],
        in_specs=[SMEM] + [VMEM] * 5,
        out_specs=[VMEM, VMEM],
        scratch_shapes=[pltpu.SMEM((listed + 1,), jnp.int32)],
        compiler_params=pltpu.CompilerParams(vmem_limit_bytes=60 * 1024 * 1024),
        name="attend_blocks",
    )(
        jnp.where(held, local, -1),
        all_q,
        passage_keys,
        passage_values,
        jnp.concatenate([cosine, cosine], axis=2),
        jnp.concatenate([-sine, sine], axis=2),
    )
    first_row = lax.axis_index("ctx") * half
    live = first_row + jnp.arange(half, dtype=jnp.int32) < row_counts[0]
    live = jnp.broadcast_to(live.astype(jnp.float32)[:, None], (half, width))
    each = owners // heads
    side = group * half
    bf16, f32 = jnp.bfloat16, jnp.float32
    more_x, more_z, more_h = max(inner - 1, 1), max(outer - 1, 1), max(heads - 1, 1)
    return pl.pallas_call(
        functools.partial(finish, owners, heads),
        out_shape=jax.ShapeDtypeStruct((1, each * half, columns), bf16),
        in_specs=[VMEM] * 4,
        out_specs=VMEM,
        scratch_shapes=[
            pltpu.VMEM((owners, width, side), f32),
            pltpu.VMEM((owners, 8, side), f32),
            pltpu.VMEM((owners, width, side), bf16),
            pltpu.VMEM((owners, 8, side), f32),
            pltpu.VMEM((more_x, outer, width, side), bf16),
            pltpu.VMEM((more_x, outer, 8, side), f32),
            pltpu.VMEM((more_z, width, side), bf16),
            pltpu.VMEM((more_z, 8, side), f32),
            pltpu.VMEM((owners, half, features), bf16),
            pltpu.VMEM((owners, half, columns), f32),
            pltpu.VMEM((owners, half, columns), bf16),
            pltpu.VMEM((more_h, each, half, columns), bf16),
            dma((2, owners)),
            dma((2, owners)),
            dma((2, more_x, outer)),
            dma((2, more_x, outer)),
            dma((2, more_z)),
            dma((2, more_z)),
            dma((owners,)),
            dma((owners,)),
            dma((owners,)),
            dma((more_h, each)),
        ],
        compiler_params=pltpu.CompilerParams(
            collective_id=1, has_side_effects=True, vmem_limit_bytes=63 * 1024 * 1024
        ),
        name="finish",
    )(acc, ml, out_weight, live)


def solution(mesh):
    return jax.shard_map(
        body,
        mesh=mesh,
        in_specs=(
            P("lib", None, "head"),
            P("lib", "ctx", "head"),
            P("lib", "ctx", "head"),
            P("lib"),
            P("head", "lib"),
            P("lib", None),
            P("lib", None),
            P("lib"),
        ),
        out_specs=P("ctx", "head", "lib"),
        check_vma=False,
    )
```

```python
import functools

import jax
import jax.numpy as jnp
from jax import lax
from jax.experimental import pallas as pl
from jax.experimental.pallas import tpu as pltpu
from jax.sharding import PartitionSpec as P

MESH = pl.DeviceIdType.MESH
VMEM = pl.BlockSpec(memory_space=pltpu.VMEM)
SMEM = pl.BlockSpec(memory_space=pltpu.SMEM)
theta_base = 500000.0
log2_e = 1.4426950408889634
lowest = -1e30


def greet(peers):
    barrier = pltpu.get_barrier_semaphore()
    for peer in peers:
        pl.semaphore_signal(barrier, inc=1, device_id=peer, device_id_type=MESH)
    pl.semaphore_wait(barrier, len(peers))


def remote(source, target, sent, landed, peer):
    return pltpu.make_async_remote_copy(
        src_ref=source,
        dst_ref=target,
        send_sem=sent,
        recv_sem=landed,
        device_id=peer,
        device_id_type=MESH,
    )


class Grid:
    def __init__(self, owners):
        self.owners = owners
        self.inner = 2 if owners % 2 == 0 else 1
        self.outer = owners // self.inner
        self.me = lax.axis_index("lib")
        self.x = lax.rem(self.me, self.inner)
        self.z = lax.div(self.me, self.inner)

    def at(self, step_z, step_x):
        z = lax.rem(self.z + step_z + self.outer, self.outer)
        x = lax.rem(self.x + step_x + self.inner, self.inner)
        return z * self.inner + x


def gather_queries(owners, q_ref, meta_ref, all_q, all_meta, own_sem, sent, landed, shared, given,
                   meta_sent, meta_landed):
    grid = Grid(owners)
    me = grid.me
    core = lax.axis_index("ctx")
    other = 1 - core
    half = q_ref.shape[1] // 2
    mine = pl.ds(pl.multiple_of(core * half, half), half)
    theirs = pl.ds(pl.multiple_of(other * half, half), half)
    greet([{"lib": lax.rem(me + d, owners)} for d in range(1, owners)] + [{"ctx": other}])

    own = pltpu.make_async_copy(q_ref.at[0], all_q.at[me], own_sem.at[0])
    own.start()
    own_meta = pltpu.make_async_copy(meta_ref, all_meta.at[me], own_sem.at[1])
    own_meta.start()
    started = []
    for d in range(1, owners):
        copy = remote(meta_ref, all_meta.at[me], meta_sent.at[d], meta_landed.at[me],
                      {"lib": lax.rem(me + d, owners)})
        copy.start()
        started.append(copy)

    def send(source, prompt, slot, target):
        copy = remote(source, all_q.at[prompt, mine, :], sent.at[slot], landed.at[prompt],
                      {"lib": target})
        copy.start()
        started.append(copy)

    def wait_landed(prompt):
        remote(all_q.at[prompt, mine, :], all_q.at[prompt, mine, :], sent.at[0],
               landed.at[prompt], {"lib": me}).wait_recv()

    def share(prompt):
        copy = remote(all_q.at[prompt, mine, :], all_q.at[prompt, mine, :], given.at[prompt],
                      shared.at[prompt], {"ctx": other})
        copy.start()
        started.append(copy)

    slot = 0
    for dz in range(1, grid.outer):
        send(q_ref.at[0, mine, :], me, slot, grid.at(dz, 0))
        slot += 1
    for dx in range(1, grid.inner):
        send(q_ref.at[0, mine, :], me, slot, grid.at(0, dx))
        slot += 1
    for dz in range(1, grid.outer):
        prompt = grid.at(-dz, 0)
        wait_landed(prompt)
        for dx in range(1, grid.inner):
            send(all_q.at[prompt, mine, :], prompt, slot, grid.at(0, dx))
            slot += 1
        share(prompt)
    for dx in range(1, grid.inner):
        for dz in range(0, grid.outer):
            prompt = grid.at(-dz, -dx)
            wait_landed(prompt)
            share(prompt)
    own.wait()
    own_meta.wait()
    for d in range(1, owners):
        prompt = lax.rem(me + d, owners)
        remote(all_q.at[prompt, theirs, :], all_q.at[prompt, theirs, :], given.at[prompt],
               shared.at[prompt], {"ctx": other}).wait_recv()
        remote(meta_ref, all_meta.at[prompt], meta_sent.at[d], meta_landed.at[prompt],
               {"lib": me}).wait_recv()
    for copy in started:
        copy.wait_send()


def attend_blocks(listed_ref, q_ref, k_ref, v_ref, cos_ref, sin_ref, acc_ref, ml_ref, order,
                  q_turned, chunk=128, sizes=(8, 4, 2, 1), depth=1):
    prompts, listed = listed_ref.shape
    rows = q_ref.shape[1]
    width = k_ref.shape[2]
    group = q_ref.shape[2] // width
    half = rows // 2
    side = group * half
    heads_each = max(1, min(group, chunk // half))
    scale = width ** (-0.5) * log2_e
    pieces = [
        (part, slice(first * half, (first + heads_each) * half), first)
        for part in range(2)
        for first in range(0, group, heads_each)
    ]

    def prompt_step(p, carry):
        def collect(k, count):
            order[count] = k
            return count + jnp.where(listed_ref[p, k] >= 0, 1, 0)

        count = lax.fori_loop(0, listed, collect, 0)
        acc_ref[p] = jnp.zeros(acc_ref.shape[1:], jnp.float32)
        place = lax.broadcasted_iota(jnp.int32, ml_ref.shape[1:], 1)
        ml_ref[p] = jnp.where(place == 0, lowest, 0.0)

        @pl.when(count > 0)
        def _():
            for part, cols, first in pieces:
                query = jnp.concatenate(
                    [
                        q_ref[p, part * half:(part + 1) * half, g * width:(g + 1) * width]
                        for g in range(first, first + heads_each)
                    ],
                    axis=0,
                )
                q_turned[part, :, cols] = query.T

        def block_step(j, carry, start, count_each):
            keys, values = [], []
            for step in range(count_each):
                entry = order[start + j * count_each + step]
                i = listed_ref[p, entry]
                block = k_ref[i].astype(jnp.float32)
                turned = pltpu.roll(block, width // 2, 1)
                keys.append(
                    (
                        block * cos_ref[p, pl.ds(entry, 1), :]
                        + turned * sin_ref[p, pl.ds(entry, 1), :]
                    ).astype(jnp.bfloat16)
                )
                values.append(v_ref[i].T)
            keys = jnp.concatenate(keys, axis=0)
            values = jnp.concatenate(values, axis=1)

            def score(index):
                part, cols, _ = pieces[index]
                return jnp.dot(keys, q_turned[part, :, cols], preferred_element_type=jnp.float32)

            states = [
                (ml_ref[p, part, 0:1, cols], ml_ref[p, part, 1:2, cols]) for part, cols, _ in pieces
            ]
            queue = [score(index) for index in range(min(depth, len(pieces)))]
            results = []
            for index, (part, cols, _) in enumerate(pieces):
                scores = queue.pop(0)
                if index + depth < len(pieces):
                    queue.append(score(index + depth))
                before, total = states[index]
                highest = jnp.maximum(before, jnp.max(scores, axis=0, keepdims=True) * scale)
                weights = jnp.exp2(scores * scale - highest)
                fade = jnp.exp2(before - highest)
                total = total * fade + jnp.sum(weights, axis=0, keepdims=True)
                summed = jnp.dot(
                    values, weights.astype(jnp.bfloat16), preferred_element_type=jnp.float32
                )
                results.append((highest, total, fade, summed))
            for (part, cols, _), (highest, total, fade, summed) in zip(pieces, results):
                ml_ref[p, part, 0:1, cols] = highest
                ml_ref[p, part, 1:2, cols] = total
                acc_ref[p, part, :, cols] = acc_ref[p, part, :, cols] * fade + summed
            return carry

        done = 0
        for count_each in sizes:
            rounds = lax.div(count - done, count_each)
            step = functools.partial(block_step, start=done, count_each=count_each)
            lax.fori_loop(0, rounds, step, 0)
            done = done + rounds * count_each
        return carry

    lax.fori_loop(0, prompts, prompt_step, 0)


def join(parts):
    highest = functools.reduce(jnp.maximum, [part[0] for part in parts])
    factors = [jnp.exp2(part[0] - highest) for part in parts]
    totals = sum(part[1] * factor for part, factor in zip(parts, factors))
    summed = sum(part[2].astype(jnp.float32) * factor for part, factor in zip(parts, factors))
    return highest, totals, summed


def finish(owners, heads, acc_ref, ml_ref, w_ref, live_ref, out_ref,
           pacc, pml, sbuf, sml, bbuf, bml, cbuf, cml, att, fbuf, pbuf, rbuf,
           a_sent, a_landed, b_sent, b_landed, c_sent, c_landed,
           d_sent, d_landed, f_sent, f_landed):
    grid = Grid(owners)
    me = grid.me
    core = lax.axis_index("ctx")
    head = lax.axis_index("head")
    other = 1 - core
    each = owners // heads
    half = att.shape[1]
    width = acc_ref.shape[2]
    group = att.shape[2] // width
    peers = [{"ctx": other}]
    peers += [{"lib": grid.at(0, dx)} for dx in range(1, grid.inner)]
    peers += [{"lib": grid.at(dz, 0)} for dz in range(1, grid.outer)]
    peers += [{"head": lax.rem(head + d, heads)} for d in range(1, heads)]
    greet(peers)
    started = []

    def launch(*args):
        copy = remote(*args)
        copy.start()
        started.append(copy)

    order = [(dz, dx) for dx in range(1, grid.inner)
             for dz in list(range(1, grid.outer)) + [0]]
    order += [(dz, 0) for dz in range(1, grid.outer)] + [(0, 0)]
    for dz, dx in order:
        p = grid.at(dz, dx)
        launch(acc_ref.at[p, other], pacc.at[p], a_sent.at[0, p], a_landed.at[0, p], {"ctx": other})
        launch(ml_ref.at[p, other], pml.at[p], a_sent.at[1, p], a_landed.at[1, p], {"ctx": other})

    def store(slot, state):
        highest, totals, summed = state
        sbuf[slot] = summed.astype(jnp.bfloat16)
        sml[slot, 0:1] = highest
        sml[slot, 1:2] = totals

    def wait_into(target, landed):
        remote(target, target, landed, landed, {"ctx": other}).wait_recv()

    slot = 0
    for dz, dx in order:
        p = grid.at(dz, dx)
        wait_into(pacc.at[p], a_landed.at[0, p])
        wait_into(pml.at[p], a_landed.at[1, p])
        parts = [
            (ml_ref[p, core, 0:1], ml_ref[p, core, 1:2], acc_ref[p, core]),
            (pml[p, 0:1], pml[p, 1:2], pacc[p]),
        ]
        if dx == 0:
            for ex in range(grid.inner - 1):
                wait_into(bbuf.at[ex, dz], b_landed.at[0, ex, dz])
                wait_into(bml.at[ex, dz], b_landed.at[1, ex, dz])
                parts.append((bml[ex, dz, 0:1], bml[ex, dz, 1:2], bbuf[ex, dz]))
        if dz == 0 and dx == 0:
            for ez in range(grid.outer - 1):
                wait_into(cbuf.at[ez], c_landed.at[0, ez])
                wait_into(cml.at[ez], c_landed.at[1, ez])
                parts.append((cml[ez, 0:1], cml[ez, 1:2], cbuf[ez]))
        state = join(parts)
        if dx != 0:
            store(slot, state)
            peer = {"lib": grid.at(0, dx)}
            launch(sbuf.at[slot], bbuf.at[dx - 1, dz], b_sent.at[0, dx - 1, dz],
                   b_landed.at[0, dx - 1, dz], peer)
            launch(sml.at[slot], bml.at[dx - 1, dz], b_sent.at[1, dx - 1, dz],
                   b_landed.at[1, dx - 1, dz], peer)
            slot += 1
        elif dz != 0:
            store(slot, state)
            peer = {"lib": p}
            launch(sbuf.at[slot], cbuf.at[dz - 1], c_sent.at[0, dz - 1], c_landed.at[0, dz - 1], peer)
            launch(sml.at[slot], cml.at[dz - 1], c_sent.at[1, dz - 1], c_landed.at[1, dz - 1], peer)
            slot += 1
        else:
            mixed = state[2] / state[1]
            for g in range(group):
                rows = mixed[:, g * half:(g + 1) * half].T
                rows = jnp.where(live_ref[...] > 0, rows, 0.0)
                att[me, :, g * width:(g + 1) * width] = rows.astype(jnp.bfloat16)

    def spread(p, slot, target):
        launch(att.at[p], att.at[p], d_sent.at[slot], d_landed.at[p], {"lib": target})

    def project(p):
        share = jnp.dot(att[p], w_ref[...], preferred_element_type=jnp.float32)
        fbuf[p] = share
        pbuf[p] = share.astype(jnp.bfloat16)
        target = lax.div(p, each)
        local = lax.rem(p, each)
        away = lax.rem(target - head + heads, heads)

        @pl.when(away != 0)
        def _():
            remote(pbuf.at[p], rbuf.at[away - 1, local], f_sent.at[p],
                   f_landed.at[away - 1, local], {"head": target}).start()

    slot = 0
    for dz in range(1, grid.outer):
        spread(me, slot, grid.at(dz, 0))
        slot += 1
    for dx in range(1, grid.inner):
        spread(me, slot, grid.at(0, dx))
        slot += 1
    project(me)
    for dz in range(1, grid.outer):
        p = grid.at(-dz, 0)
        wait_into(att.at[p], d_landed.at[p])
        for dx in range(1, grid.inner):
            spread(p, slot, grid.at(0, dx))
            slot += 1
        project(p)
    for dx in range(1, grid.inner):
        for dz in range(grid.outer):
            p = grid.at(-dz, -dx)
            wait_into(att.at[p], d_landed.at[p])
            project(p)
    for local in range(each):
        p = head * each + local
        total = fbuf[p]
        for away in range(heads - 1):
            wait_into(rbuf.at[away, local], f_landed.at[away, local])
            total = total + rbuf[away, local].astype(jnp.float32)
        out_ref[0, local * half:(local + 1) * half] = total.astype(out_ref.dtype)
    for copy in started:
        copy.wait_send()
    for p in range(owners):
        @pl.when(p // each != head)
        def _():
            remote(pbuf.at[p], rbuf.at[0, 0], f_sent.at[p], f_sent.at[p], {"ctx": other}).wait_send()


def body(
    queries, passage_keys, passage_values, offsets, out_weight, passage_list, targets, row_counts
):
    owners = lax.axis_size("lib")
    heads = lax.axis_size("head")
    me = lax.axis_index("lib")
    pass_dev, _, width = passage_keys.shape
    listed = passage_list.shape[1]
    rows, features = queries.shape[1:]
    group = features // width
    half = rows // 2
    columns = out_weight.shape[1]
    inner = 2 if owners % 2 == 0 else 1
    outer = owners // inner
    dma = pltpu.SemaphoreType.DMA
    lanes = 128
    meta = jnp.pad(jnp.concatenate([passage_list, targets], axis=1), ((0, 0), (0, lanes - 2 * listed)))
    all_q, all_meta = pl.pallas_call(
        functools.partial(gather_queries, owners),
        out_shape=[
            jax.ShapeDtypeStruct((owners, rows, features), queries.dtype),
            jax.ShapeDtypeStruct((owners, 1, lanes), jnp.int32),
        ],
        in_specs=[VMEM, VMEM],
        out_specs=[VMEM, VMEM],
        scratch_shapes=[
            dma((2,)),
            dma((owners,)),
            dma((owners,)),
            dma((owners,)),
            dma((owners,)),
            dma((owners,)),
            dma((owners,)),
        ],
        compiler_params=pltpu.CompilerParams(collective_id=0, has_side_effects=True),
        name="gather_queries",
    )(queries, meta)
    chosen = all_meta[:, 0, :listed]
    local = chosen - me * pass_dev
    held = (local >= 0) & (local < pass_dev)
    lookup = local[:, :, None] == jnp.arange(pass_dev, dtype=jnp.int32)
    shift = all_meta[:, 0, listed:2 * listed] - jnp.sum(jnp.where(lookup, offsets, 0), axis=2)
    inverse = theta_base ** (-2.0 * jnp.arange(width // 2, dtype=jnp.float32) / width)
    angle = shift.astype(jnp.float32)[:, :, None] * inverse
    cosine = jnp.cos(angle)
    sine = jnp.sin(angle)
    acc, ml = pl.pallas_call(
        attend_blocks,
        out_shape=[
            jax.ShapeDtypeStruct((owners, 2, width, group * half), jnp.float32),
            jax.ShapeDtypeStruct((owners, 2, 8, group * half), jnp.float32),
        ],
        in_specs=[SMEM] + [VMEM] * 5,
        out_specs=[VMEM, VMEM],
        scratch_shapes=[
            pltpu.SMEM((listed + 1,), jnp.int32),
            pltpu.VMEM((2, width, group * half), jnp.bfloat16),
        ],
        compiler_params=pltpu.CompilerParams(vmem_limit_bytes=60 * 1024 * 1024),
        name="attend_blocks",
    )(
        jnp.where(held, local, -1),
        all_q,
        passage_keys,
        passage_values,
        jnp.concatenate([cosine, cosine], axis=2),
        jnp.concatenate([-sine, sine], axis=2),
    )
    first_row = lax.axis_index("ctx") * half
    live = first_row + jnp.arange(half, dtype=jnp.int32) < row_counts[0]
    live = jnp.broadcast_to(live.astype(jnp.float32)[:, None], (half, width))
    each = owners // heads
    side = group * half
    bf16, f32 = jnp.bfloat16, jnp.float32
    more_x, more_z, more_h = max(inner - 1, 1), max(outer - 1, 1), max(heads - 1, 1)
    return pl.pallas_call(
        functools.partial(finish, owners, heads),
        out_shape=jax.ShapeDtypeStruct((1, each * half, columns), bf16),
        in_specs=[VMEM] * 4,
        out_specs=VMEM,
        scratch_shapes=[
            pltpu.VMEM((owners, width, side), f32),
            pltpu.VMEM((owners, 8, side), f32),
            pltpu.VMEM((owners, width, side), bf16),
            pltpu.VMEM((owners, 8, side), f32),
            pltpu.VMEM((more_x, outer, width, side), bf16),
            pltpu.VMEM((more_x, outer, 8, side), f32),
            pltpu.VMEM((more_z, width, side), bf16),
            pltpu.VMEM((more_z, 8, side), f32),
            pltpu.VMEM((owners, half, features), bf16),
            pltpu.VMEM((owners, half, columns), f32),
            pltpu.VMEM((owners, half, columns), bf16),
            pltpu.VMEM((more_h, each, half, columns), bf16),
            dma((2, owners)),
            dma((2, owners)),
            dma((2, more_x, outer)),
            dma((2, more_x, outer)),
            dma((2, more_z)),
            dma((2, more_z)),
            dma((owners,)),
            dma((owners,)),
            dma((owners,)),
            dma((more_h, each)),
        ],
        compiler_params=pltpu.CompilerParams(
            collective_id=1, has_side_effects=True, vmem_limit_bytes=63 * 1024 * 1024
        ),
        name="finish",
    )(acc, ml, out_weight, live)


def solution(mesh):
    return jax.shard_map(
        body,
        mesh=mesh,
        in_specs=(
            P("lib", None, "head"),
            P("lib", "ctx", "head"),
            P("lib", "ctx", "head"),
            P("lib"),
            P("head", "lib"),
            P("lib", None),
            P("lib", None),
            P("lib"),
        ),
        out_specs=P("ctx", "head", "lib"),
        check_vma=False,
    )
```

```python
import functools

import jax
import jax.numpy as jnp
from jax import lax
from jax.experimental import pallas as pl
from jax.experimental.pallas import tpu as pltpu
from jax.sharding import PartitionSpec as P

MESH = pl.DeviceIdType.MESH
VMEM = pl.BlockSpec(memory_space=pltpu.VMEM)
SMEM = pl.BlockSpec(memory_space=pltpu.SMEM)
theta_base = 500000.0
log2_e = 1.4426950408889634
lowest = -1e30


def greet(peers):
    barrier = pltpu.get_barrier_semaphore()
    for peer in peers:
        pl.semaphore_signal(barrier, inc=1, device_id=peer, device_id_type=MESH)
    pl.semaphore_wait(barrier, len(peers))


def remote(source, target, sent, landed, peer):
    return pltpu.make_async_remote_copy(
        src_ref=source,
        dst_ref=target,
        send_sem=sent,
        recv_sem=landed,
        device_id=peer,
        device_id_type=MESH,
    )


class Grid:
    def __init__(self, owners):
        self.owners = owners
        self.inner = 2 if owners % 2 == 0 else 1
        self.outer = owners // self.inner
        self.me = lax.axis_index("lib")
        self.x = lax.rem(self.me, self.inner)
        self.z = lax.div(self.me, self.inner)

    def inside(self, step_z):
        return (self.z + step_z >= 0) & (self.z + step_z < self.outer)

    def at(self, step_z, step_x):
        z = lax.rem(self.z + step_z + self.outer, self.outer)
        x = lax.rem(self.x + step_x + self.inner, self.inner)
        return z * self.inner + x


def gather_queries(owners, q_ref, meta_ref, all_q, all_meta, own_sem, sent, landed, shared, given,
                   meta_sent, meta_landed):
    grid = Grid(owners)
    me = grid.me
    core = lax.axis_index("ctx")
    other = 1 - core
    half = q_ref.shape[1] // 2
    mine = pl.ds(pl.multiple_of(core * half, half), half)
    theirs = pl.ds(pl.multiple_of(other * half, half), half)
    greet([{"lib": lax.rem(me + d, owners)} for d in range(1, owners)] + [{"ctx": other}])

    own = pltpu.make_async_copy(q_ref.at[0], all_q.at[me], own_sem.at[0])
    own.start()
    own_meta = pltpu.make_async_copy(meta_ref, all_meta.at[me], own_sem.at[1])
    own_meta.start()
    started = []
    for d in range(1, owners):
        copy = remote(meta_ref, all_meta.at[me], meta_sent.at[d], meta_landed.at[me],
                      {"lib": lax.rem(me + d, owners)})
        copy.start()
        started.append((me >= 0, copy))

    def begin(valid, copy):
        started.append((valid, copy))

        @pl.when(valid)
        def _():
            copy.start()

    def send(valid, source, prompt, kind, target):
        begin(valid, remote(source, all_q.at[prompt, mine, :], sent.at[kind, prompt],
                            landed.at[prompt], {"lib": target}))

    def wait_landed(prompt):
        remote(all_q.at[prompt, mine, :], all_q.at[prompt, mine, :], sent.at[0, prompt],
               landed.at[prompt], {"lib": me}).wait_recv()

    def share(valid, prompt):
        begin(valid, remote(all_q.at[prompt, mine, :], all_q.at[prompt, mine, :],
                            given.at[prompt], shared.at[prompt], {"ctx": other}))

    for kind, sign in ((0, 1), (1, -1)):
        send(grid.inside(sign), q_ref.at[0, mine, :], me, kind, grid.at(sign, 0))
    for dx in range(1, grid.inner):
        send(me >= 0, q_ref.at[0, mine, :], me, 1 + dx, grid.at(0, dx))
    for far in range(1, grid.outer):
        for sign in (-1, 1):
            prompt = grid.at(sign * far, 0)
            here = grid.inside(sign * far)

            @pl.when(here)
            def _():
                wait_landed(prompt)

            send(here & grid.inside(-sign), all_q.at[prompt, mine, :], prompt, 0, grid.at(-sign, 0))
            for dx in range(1, grid.inner):
                send(here, all_q.at[prompt, mine, :], prompt, 1 + dx, grid.at(0, dx))
            share(here, prompt)
    for dx in range(1, grid.inner):
        share_from = [(me >= 0, 0)]
        for far in range(1, grid.outer):
            share_from += [(grid.inside(-far), -far), (grid.inside(far), far)]
        for here, dz in share_from:
            prompt = grid.at(dz, -dx)

            @pl.when(here)
            def _():
                wait_landed(prompt)

            share(here, prompt)
    own.wait()
    own_meta.wait()
    for d in range(1, owners):
        prompt = lax.rem(me + d, owners)
        remote(all_q.at[prompt, theirs, :], all_q.at[prompt, theirs, :], given.at[prompt],
               shared.at[prompt], {"ctx": other}).wait_recv()
        remote(meta_ref, all_meta.at[prompt], meta_sent.at[d], meta_landed.at[prompt],
               {"lib": me}).wait_recv()
    for valid, copy in started:
        @pl.when(valid)
        def _():
            copy.wait_send()


def attend_blocks(listed_ref, q_ref, k_ref, v_ref, cos_ref, sin_ref, acc_ref, ml_ref, order,
                  q_turned, chunk=128, sizes=(8, 4, 2, 1), depth=1):
    prompts, listed = listed_ref.shape
    rows = q_ref.shape[1]
    width = k_ref.shape[2]
    group = q_ref.shape[2] // width
    half = rows // 2
    side = group * half
    heads_each = max(1, min(group, chunk // half))
    scale = width ** (-0.5) * log2_e
    pieces = [
        (part, slice(first * half, (first + heads_each) * half), first)
        for part in range(2)
        for first in range(0, group, heads_each)
    ]

    def prompt_step(p, carry):
        def collect(k, count):
            order[count] = k
            return count + jnp.where(listed_ref[p, k] >= 0, 1, 0)

        count = lax.fori_loop(0, listed, collect, 0)
        acc_ref[p] = jnp.zeros(acc_ref.shape[1:], jnp.float32)
        place = lax.broadcasted_iota(jnp.int32, ml_ref.shape[1:], 1)
        ml_ref[p] = jnp.where(place == 0, lowest, 0.0)

        @pl.when(count > 0)
        def _():
            for part, cols, first in pieces:
                query = jnp.concatenate(
                    [
                        q_ref[p, part * half:(part + 1) * half, g * width:(g + 1) * width]
                        for g in range(first, first + heads_each)
                    ],
                    axis=0,
                )
                q_turned[part, :, cols] = query.T

        def block_step(j, carry, start, count_each):
            keys, values = [], []
            for step in range(count_each):
                entry = order[start + j * count_each + step]
                i = listed_ref[p, entry]
                block = k_ref[i].astype(jnp.float32)
                turned = pltpu.roll(block, width // 2, 1)
                keys.append(
                    (
                        block * cos_ref[p, pl.ds(entry, 1), :]
                        + turned * sin_ref[p, pl.ds(entry, 1), :]
                    ).astype(jnp.bfloat16)
                )
                values.append(v_ref[i].T)
            keys = jnp.concatenate(keys, axis=0)
            values = jnp.concatenate(values, axis=1)

            def score(index):
                part, cols, _ = pieces[index]
                return jnp.dot(keys, q_turned[part, :, cols], preferred_element_type=jnp.float32)

            states = [
                (ml_ref[p, part, 0:1, cols], ml_ref[p, part, 1:2, cols]) for part, cols, _ in pieces
            ]
            queue = [score(index) for index in range(min(depth, len(pieces)))]
            results = []
            for index, (part, cols, _) in enumerate(pieces):
                scores = queue.pop(0)
                if index + depth < len(pieces):
                    queue.append(score(index + depth))
                before, total = states[index]
                highest = jnp.maximum(before, jnp.max(scores, axis=0, keepdims=True) * scale)
                weights = jnp.exp2(scores * scale - highest)
                fade = jnp.exp2(before - highest)
                total = total * fade + jnp.sum(weights, axis=0, keepdims=True)
                summed = jnp.dot(
                    values, weights.astype(jnp.bfloat16), preferred_element_type=jnp.float32
                )
                results.append((highest, total, fade, summed))
            for (part, cols, _), (highest, total, fade, summed) in zip(pieces, results):
                ml_ref[p, part, 0:1, cols] = highest
                ml_ref[p, part, 1:2, cols] = total
                acc_ref[p, part, :, cols] = acc_ref[p, part, :, cols] * fade + summed
            return carry

        done = 0
        for count_each in sizes:
            rounds = lax.div(count - done, count_each)
            step = functools.partial(block_step, start=done, count_each=count_each)
            lax.fori_loop(0, rounds, step, 0)
            done = done + rounds * count_each
        return carry

    lax.fori_loop(0, prompts, prompt_step, 0)


def join(parts):
    highest = functools.reduce(jnp.maximum, [part[0] for part in parts])
    factors = [jnp.exp2(part[0] - highest) for part in parts]
    totals = sum(part[1] * factor for part, factor in zip(parts, factors))
    summed = sum(part[2].astype(jnp.float32) * factor for part, factor in zip(parts, factors))
    return highest, totals, summed


def finish(owners, heads, acc_ref, ml_ref, w_ref, live_ref, out_ref,
           pacc, pml, sbuf, sml, bbuf, bml, cbuf, cml, att, fbuf, pbuf, rbuf,
           a_sent, a_landed, b_sent, b_landed, c_sent, c_landed,
           d_sent, d_landed, f_sent, f_landed):
    grid = Grid(owners)
    me = grid.me
    core = lax.axis_index("ctx")
    head = lax.axis_index("head")
    other = 1 - core
    each = owners // heads
    half = att.shape[1]
    width = acc_ref.shape[2]
    group = att.shape[2] // width
    peers = [{"ctx": other}]
    peers += [{"lib": grid.at(0, dx)} for dx in range(1, grid.inner)]
    peers += [{"lib": grid.at(dz, 0)} for dz in range(1, grid.outer)]
    peers += [{"head": lax.rem(head + d, heads)} for d in range(1, heads)]
    greet(peers)
    started = []

    def launch(*args):
        copy = remote(*args)
        copy.start()
        started.append(copy)

    order = [(dz, dx) for dx in range(1, grid.inner)
             for dz in list(range(1, grid.outer)) + [0]]
    order += [(dz, 0) for dz in range(1, grid.outer)] + [(0, 0)]
    for dz, dx in order:
        p = grid.at(dz, dx)
        launch(acc_ref.at[p, other], pacc.at[p], a_sent.at[0, p], a_landed.at[0, p], {"ctx": other})
        launch(ml_ref.at[p, other], pml.at[p], a_sent.at[1, p], a_landed.at[1, p], {"ctx": other})

    def store(slot, state):
        highest, totals, summed = state
        sbuf[slot] = summed.astype(jnp.bfloat16)
        sml[slot, 0:1] = highest
        sml[slot, 1:2] = totals

    def wait_into(target, landed):
        remote(target, target, landed, landed, {"ctx": other}).wait_recv()

    slot = 0
    for dz, dx in order:
        p = grid.at(dz, dx)
        wait_into(pacc.at[p], a_landed.at[0, p])
        wait_into(pml.at[p], a_landed.at[1, p])
        parts = [
            (ml_ref[p, core, 0:1], ml_ref[p, core, 1:2], acc_ref[p, core]),
            (pml[p, 0:1], pml[p, 1:2], pacc[p]),
        ]
        if dx == 0:
            for ex in range(grid.inner - 1):
                wait_into(bbuf.at[ex, dz], b_landed.at[0, ex, dz])
                wait_into(bml.at[ex, dz], b_landed.at[1, ex, dz])
                parts.append((bml[ex, dz, 0:1], bml[ex, dz, 1:2], bbuf[ex, dz]))
        if dz == 0 and dx == 0:
            for ez in range(grid.outer - 1):
                wait_into(cbuf.at[ez], c_landed.at[0, ez])
                wait_into(cml.at[ez], c_landed.at[1, ez])
                parts.append((cml[ez, 0:1], cml[ez, 1:2], cbuf[ez]))
        state = join(parts)
        if dx != 0:
            store(slot, state)
            peer = {"lib": grid.at(0, dx)}
            launch(sbuf.at[slot], bbuf.at[dx - 1, dz], b_sent.at[0, dx - 1, dz],
                   b_landed.at[0, dx - 1, dz], peer)
            launch(sml.at[slot], bml.at[dx - 1, dz], b_sent.at[1, dx - 1, dz],
                   b_landed.at[1, dx - 1, dz], peer)
            slot += 1
        elif dz != 0:
            store(slot, state)
            peer = {"lib": p}
            launch(sbuf.at[slot], cbuf.at[dz - 1], c_sent.at[0, dz - 1], c_landed.at[0, dz - 1], peer)
            launch(sml.at[slot], cml.at[dz - 1], c_sent.at[1, dz - 1], c_landed.at[1, dz - 1], peer)
            slot += 1
        else:
            mixed = state[2] / state[1]
            for g in range(group):
                rows = mixed[:, g * half:(g + 1) * half].T
                rows = jnp.where(live_ref[...] > 0, rows, 0.0)
                att[me, :, g * width:(g + 1) * width] = rows.astype(jnp.bfloat16)

    spreads = []

    def spread(valid, p, kind, target):
        copy = remote(att.at[p], att.at[p], d_sent.at[kind, p], d_landed.at[p], {"lib": target})
        spreads.append((valid, copy))

        @pl.when(valid)
        def _():
            copy.start()

    def project(p):
        share = jnp.dot(att[p], w_ref[...], preferred_element_type=jnp.float32)
        fbuf[p] = share
        pbuf[p] = share.astype(jnp.bfloat16)
        target = lax.div(p, each)
        local = lax.rem(p, each)
        away = lax.rem(target - head + heads, heads)

        @pl.when(away != 0)
        def _():
            remote(pbuf.at[p], rbuf.at[away - 1, local], f_sent.at[p],
                   f_landed.at[away - 1, local], {"head": target}).start()

    for kind, sign in ((0, 1), (1, -1)):
        spread(grid.inside(sign), me, kind, grid.at(sign, 0))
    for dx in range(1, grid.inner):
        spread(me >= 0, me, 1 + dx, grid.at(0, dx))
    project(me)
    for far in range(1, grid.outer):
        for sign in (-1, 1):
            p = grid.at(sign * far, 0)
            here = grid.inside(sign * far)

            @pl.when(here)
            def _():
                wait_into(att.at[p], d_landed.at[p])

            spread(here & grid.inside(-sign), p, 0, grid.at(-sign, 0))
            for dx in range(1, grid.inner):
                spread(here, p, 1 + dx, grid.at(0, dx))

            @pl.when(here)
            def _():
                project(p)
    for dx in range(1, grid.inner):
        arrivals = [(me >= 0, 0)]
        for far in range(1, grid.outer):
            arrivals += [(grid.inside(-far), -far), (grid.inside(far), far)]
        for here, dz in arrivals:
            p = grid.at(dz, -dx)

            @pl.when(here)
            def _():
                wait_into(att.at[p], d_landed.at[p])
                project(p)
    for local in range(each):
        p = head * each + local
        total = fbuf[p]
        for away in range(heads - 1):
            wait_into(rbuf.at[away, local], f_landed.at[away, local])
            total = total + rbuf[away, local].astype(jnp.float32)
        out_ref[0, local * half:(local + 1) * half] = total.astype(out_ref.dtype)
    for copy in started:
        copy.wait_send()
    for valid, copy in spreads:
        @pl.when(valid)
        def _():
            copy.wait_send()
    for p in range(owners):
        @pl.when(p // each != head)
        def _():
            remote(pbuf.at[p], rbuf.at[0, 0], f_sent.at[p], f_sent.at[p], {"ctx": other}).wait_send()


def body(
    queries, passage_keys, passage_values, offsets, out_weight, passage_list, targets, row_counts
):
    owners = lax.axis_size("lib")
    heads = lax.axis_size("head")
    me = lax.axis_index("lib")
    pass_dev, _, width = passage_keys.shape
    listed = passage_list.shape[1]
    rows, features = queries.shape[1:]
    group = features // width
    half = rows // 2
    columns = out_weight.shape[1]
    inner = 2 if owners % 2 == 0 else 1
    outer = owners // inner
    dma = pltpu.SemaphoreType.DMA
    lanes = 128
    meta = jnp.pad(jnp.concatenate([passage_list, targets], axis=1), ((0, 0), (0, lanes - 2 * listed)))
    all_q, all_meta = pl.pallas_call(
        functools.partial(gather_queries, owners),
        out_shape=[
            jax.ShapeDtypeStruct((owners, rows, features), queries.dtype),
            jax.ShapeDtypeStruct((owners, 1, lanes), jnp.int32),
        ],
        in_specs=[VMEM, VMEM],
        out_specs=[VMEM, VMEM],
        scratch_shapes=[
            dma((2,)),
            dma((inner + 1, owners)),
            dma((owners,)),
            dma((owners,)),
            dma((owners,)),
            dma((owners,)),
            dma((owners,)),
        ],
        compiler_params=pltpu.CompilerParams(collective_id=0, has_side_effects=True),
        name="gather_queries",
    )(queries, meta)
    chosen = all_meta[:, 0, :listed]
    local = chosen - me * pass_dev
    held = (local >= 0) & (local < pass_dev)
    lookup = local[:, :, None] == jnp.arange(pass_dev, dtype=jnp.int32)
    shift = all_meta[:, 0, listed:2 * listed] - jnp.sum(jnp.where(lookup, offsets, 0), axis=2)
    inverse = theta_base ** (-2.0 * jnp.arange(width // 2, dtype=jnp.float32) / width)
    angle = shift.astype(jnp.float32)[:, :, None] * inverse
    cosine = jnp.cos(angle)
    sine = jnp.sin(angle)
    acc, ml = pl.pallas_call(
        attend_blocks,
        out_shape=[
            jax.ShapeDtypeStruct((owners, 2, width, group * half), jnp.float32),
            jax.ShapeDtypeStruct((owners, 2, 8, group * half), jnp.float32),
        ],
        in_specs=[SMEM] + [VMEM] * 5,
        out_specs=[VMEM, VMEM],
        scratch_shapes=[
            pltpu.SMEM((listed + 1,), jnp.int32),
            pltpu.VMEM((2, width, group * half), jnp.bfloat16),
        ],
        compiler_params=pltpu.CompilerParams(vmem_limit_bytes=60 * 1024 * 1024),
        name="attend_blocks",
    )(
        jnp.where(held, local, -1),
        all_q,
        passage_keys,
        passage_values,
        jnp.concatenate([cosine, cosine], axis=2),
        jnp.concatenate([-sine, sine], axis=2),
    )
    first_row = lax.axis_index("ctx") * half
    live = first_row + jnp.arange(half, dtype=jnp.int32) < row_counts[0]
    live = jnp.broadcast_to(live.astype(jnp.float32)[:, None], (half, width))
    each = owners // heads
    side = group * half
    bf16, f32 = jnp.bfloat16, jnp.float32
    more_x, more_z, more_h = max(inner - 1, 1), max(outer - 1, 1), max(heads - 1, 1)
    return pl.pallas_call(
        functools.partial(finish, owners, heads),
        out_shape=jax.ShapeDtypeStruct((1, each * half, columns), bf16),
        in_specs=[VMEM] * 4,
        out_specs=VMEM,
        scratch_shapes=[
            pltpu.VMEM((owners, width, side), f32),
            pltpu.VMEM((owners, 8, side), f32),
            pltpu.VMEM((owners, width, side), bf16),
            pltpu.VMEM((owners, 8, side), f32),
            pltpu.VMEM((more_x, outer, width, side), bf16),
            pltpu.VMEM((more_x, outer, 8, side), f32),
            pltpu.VMEM((more_z, width, side), bf16),
            pltpu.VMEM((more_z, 8, side), f32),
            pltpu.VMEM((owners, half, features), bf16),
            pltpu.VMEM((owners, half, columns), f32),
            pltpu.VMEM((owners, half, columns), bf16),
            pltpu.VMEM((more_h, each, half, columns), bf16),
            dma((2, owners)),
            dma((2, owners)),
            dma((2, more_x, outer)),
            dma((2, more_x, outer)),
            dma((2, more_z)),
            dma((2, more_z)),
            dma((inner + 1, owners)),
            dma((owners,)),
            dma((owners,)),
            dma((more_h, each)),
        ],
        compiler_params=pltpu.CompilerParams(
            collective_id=1, has_side_effects=True, vmem_limit_bytes=63 * 1024 * 1024
        ),
        name="finish",
    )(acc, ml, out_weight, live)


def solution(mesh):
    return jax.shard_map(
        body,
        mesh=mesh,
        in_specs=(
            P("lib", None, "head"),
            P("lib", "ctx", "head"),
            P("lib", "ctx", "head"),
            P("lib"),
            P("head", "lib"),
            P("lib", None),
            P("lib", None),
            P("lib"),
        ),
        out_specs=P("ctx", "head", "lib"),
        check_vma=False,
    )
```
